512 devices in a mesh: row: 16 (over y, core), col: 32 (over z, x).
Axes of the slice: x: 4, y: 8, z: 8, core: 2. Of those that a mesh axis runs over, the one named last changes fastest.
Arguments:
- foreground: int32 [4096, 16384], P('row', 'col'), may hold values 0 or 1
- seed_keys: float32 [4096, 16384], P('row', 'col'), may hold values from 1 to 2
Outputs:
- labels: float32 [4096, 16384], P('row', 'col')
The draws below stay inside these ranges and needn't reach their ends.
All inputs are finite; a program needn't handle non-finite values. No bound on the sum of `foreground` on one device may be relied on, other than what follows from the above.
Results may differ from the reference program's by a relative error of at most 0.0003.
Values sent between devices are 32-bit elements; how exact they have to be, the bound alone decides.
A program may use at most 64 MiB of HBM per device.

```python
import jax
import jax.numpy as jnp
from jax import lax

SWEEPS = 48
NR = 4096
NW = 16384


def touch_ends(values, stream_key, low, largest):
    place = [jax.random.randint(jax.random.fold_in(stream_key, axis), (), 0, length) for axis, length in enumerate(values.shape)]
    main_axis = values.shape.index(max(values.shape))
    neighbour = place[:main_axis] + [(place[main_axis] + 1) % values.shape[main_axis]] + place[main_axis + 1:]
    return values.at[tuple(place)].set(low).at[tuple(neighbour)].set(largest)


def shard_levels(key, extent, pieces, least, top_value):
    def one(axis_at, shards_of):
        heights = jax.random.uniform(jax.random.fold_in(jax.random.fold_in(key, 6), axis_at), (shards_of,), jnp.float32, least / len(pieces), top_value / len(pieces))
        return jnp.repeat(jnp.exp(heights), extent[axis_at] // shards_of).reshape((-1,) + (1,) * (len(extent) - axis_at - 1))

    level = one(*pieces[0])
    for cut in pieces[1:]:
        level = level * one(*cut)
    return level


def setup_inputs(seed: int = 0) -> dict:
    keys = jax.random.split(jax.random.key(seed), 3)
    return {
        "foreground": touch_ends((jax.random.randint(keys[0], (NR, NW), 0, 5) < 2).astype(jnp.int32), jax.random.fold_in(keys[0], 1), 0, 1),
        "seed_keys": jnp.clip(1.0 + 1.0 * jax.random.uniform(keys[1], (NR, NW), jnp.float32) ** shard_levels(keys[1], (NR, NW), ((0, 16), (1, 32)), -0.2, 0.2), 1.0, 2.0),
    }


absent_label = 1.0e30


def sweep_once(padded):
    height = padded.shape[0] - 2
    breadth = padded.shape[1] - 2
    center = padded[1:1 + height, 1:1 + breadth]
    filled = jnp.where(padded > 0, padded, jnp.full_like(padded, absent_label))
    smallest = filled[1:1 + height, 1:1 + breadth]
    for offset_row in range(3):
        for offset_col in range(3):
            smallest = jnp.minimum(smallest, filled[offset_row:offset_row + height, offset_col:offset_col + breadth])
    return jnp.where(center > 0, smallest, jnp.zeros_like(center))


def reference(foreground, seed_keys):
    current = jnp.where(foreground == 1, seed_keys, jnp.zeros_like(seed_keys))

    def advance(sweep_index, present):
        return sweep_once(jnp.pad(present, 1))

    current = lax.fori_loop(0, SWEEPS, advance, current)
    return current
```

```python
import functools

import jax
import jax.numpy as jnp
from jax import lax
from jax.experimental import pallas as pl
from jax.experimental.pallas import tpu as pltpu
from jax.sharding import PartitionSpec as P

SWEEPS = 48
SCALE = 240.0
SHIFT = 360.0
BIG = 2.0**126
EDGE = 2.0**125
LANES = 128
HALF = 64
ROWS = 256
COLS = 512
WIDE = ROWS + 2 * SWEEPS
BLOCKS = 16
STEPS = WIDE // BLOCKS
LSTEPS = 5
UNROLL = 12
DIRECTIONS = ((-1, -1), (-1, 1), (1, -1), (1, 1), (0, -1), (0, 1), (-1, 0), (1, 0))


def exchange_kernel(fg_hbm, key_hbm, ext, sides, corners, fg, key, packed, load_sem, send_sem, recv_sem):
    row, col = lax.axis_index("row"), lax.axis_index("col")
    rows, cols = lax.axis_size("row"), lax.axis_size("col")
    loads = [
        pltpu.make_async_copy(fg_hbm, fg, load_sem.at[0]),
        pltpu.make_async_copy(key_hbm, key, load_sem.at[1]),
    ]
    for load in loads:
        load.start()

    def present(dr, dc):
        r, c = row + dr, col + dc
        return (r >= 0) & (r < rows) & (c >= 0) & (c < cols)

    barrier = pltpu.get_barrier_semaphore()
    for dr, dc in DIRECTIONS:

        @pl.when(present(dr, dc))
        def _():
            pl.semaphore_signal(
                barrier, inc=1, device_id=(row + dr, col + dc), device_id_type=pl.DeviceIdType.MESH
            )

    for load in loads:
        load.wait()
    ext[:ROWS, :] = jnp.where(fg[...] == 1, jnp.exp2(key[...] * SCALE - SHIFT), BIG)
    low = lax.broadcasted_iota(jnp.int32, (ROWS // 2, LANES), 1) < HALF
    top, bottom = slice(0, ROWS // 2), slice(ROWS // 2, ROWS)
    packed[0] = jnp.where(low, ext[top, :LANES], pltpu.roll(ext[bottom, :LANES], HALF, 1))
    packed[1] = jnp.where(low, pltpu.roll(ext[bottom, COLS - LANES :], HALF, 1), ext[top, COLS - LANES :])

    heights = {-1: pl.ds(0, SWEEPS), 1: pl.ds(ROWS - SWEEPS, SWEEPS)}
    widths = {-1: pl.ds(0, LANES), 1: pl.ds(COLS - LANES, LANES)}
    halos = {-1: pl.ds(ROWS, SWEEPS), 1: pl.ds(ROWS + SWEEPS, SWEEPS)}

    def ends(dr, dc):
        if dr == 0:
            at = 0 if dc < 0 else 1
            return packed.at[at], sides.at[at]
        if dc == 0:
            return ext.at[heights[dr]], ext.at[halos[dr]]
        return ext.at[heights[dr], widths[dc]], corners.at[(1 + dr) + (1 + dc) // 2]

    copies = []
    for i, (dr, dc) in enumerate(DIRECTIONS):
        src, dst = ends(dr, dc)
        copies.append(
            pltpu.make_async_remote_copy(
                src_ref=src,
                dst_ref=dst,
                send_sem=send_sem.at[i],
                recv_sem=recv_sem.at[i],
                device_id=(row + dr, col + dc),
                device_id_type=pl.DeviceIdType.MESH,
            )
        )
    count = jnp.int32(0)
    for dr, dc in DIRECTIONS:
        count += jnp.where(present(dr, dc), 1, 0)
    pl.semaphore_wait(barrier, count)
    for (dr, dc), copy in zip(DIRECTIONS, copies):
        pl.when(present(dr, dc))(copy.start)
    for (dr, dc), copy in zip(DIRECTIONS, copies):

        @pl.when(jnp.logical_not(present(-dr, -dc)))
        def _():
            dst = ends(dr, dc)[1]
            dst[...] = jnp.full(dst.shape, BIG, jnp.float32)

    for (dr, dc), copy in zip(DIRECTIONS, copies):
        pl.when(present(-dr, -dc))(copy.wait_recv)
    for (dr, dc), copy in zip(DIRECTIONS, copies):
        pl.when(present(dr, dc))(copy.wait_send)


def sweep_kernel(ext, sides, corners, out, flat, state, mask, turned):
    lane = lax.broadcasted_iota(jnp.int32, (8, LANES), 1)
    low = lane < HALF
    picks = [(lane * LSTEPS + j) & (LANES - 1) for j in range(LSTEPS)]
    for g in range(WIDE // 8):
        at = slice(8 * g, 8 * g + 8)
        if 8 * g < ROWS // 2:
            side = jnp.where(low, sides[0, at], sides[1, at])
        elif 8 * g < ROWS:
            lower = slice(8 * g - ROWS // 2, 8 * g - ROWS // 2 + 8)
            side = pltpu.roll(jnp.where(low, sides[1, lower], sides[0, lower]), HALF, 1)
        else:
            below = 8 * g < ROWS + SWEEPS
            start = 8 * g - (ROWS if below else ROWS + SWEEPS)
            first = 0 if below else 2
            at_corner = slice(start, start + 8)
            side = jnp.where(low, corners[first, at_corner], corners[first + 1, at_corner])
        sources = [ext[at, LANES * t : LANES * t + LANES] for t in range(4)] + [side]
        for j in range(LSTEPS):
            value = jnp.take_along_axis(sources[0], picks[j], axis=1)
            for t in range(1, LSTEPS):
                first_lane = -(-(LANES * t - j) // LSTEPS)
                value = jnp.where(lane < first_lane, value, jnp.take_along_axis(sources[t], picks[j], axis=1))
            flat[j, at] = value
    big = jnp.full((BLOCKS, LANES), BIG, jnp.bfloat16)
    zero = jnp.zeros((BLOCKS, LANES), jnp.bfloat16)

    def turn(k, first, last):
        turned[k, 0] = pltpu.roll(last, 1, 1)
        turned[k, 1] = pltpu.roll(first, LANES - 1, 1)

    for k in range(STEPS):
        values = [flat[j, pl.ds(k, BLOCKS, stride=STEPS), :].astype(jnp.bfloat16) for j in range(LSTEPS)]
        for j in range(LSTEPS):
            state[k, j] = values[j]
            mask[k, j] = jnp.where(values[j] >= EDGE, big, zero)
        turn(k, values[0], values[-1])

    def across(k):
        a = [state[k, j] for j in range(LSTEPS)]
        p, q = jnp.minimum(a[0], a[1]), jnp.minimum(a[2], a[3])
        return [
            jnp.minimum(turned[k, 0], p),
            jnp.minimum(p, a[2]),
            jnp.minimum(a[1], q),
            jnp.minimum(q, a[4]),
            jnp.minimum(jnp.minimum(a[3], a[4]), turned[k, 1]),
        ]

    def sweeps(i, carry):
        for u in range(UNROLL):
            begin = 2 * u % STEPS
            before = across((begin - 1) % STEPS)
            here = begin_row = across(begin)
            for pair in range(STEPS // 2):
                k = (begin + 2 * pair) % STEPS
                after = across(k + 1)
                follow = begin_row if pair == STEPS // 2 - 1 else across((k + 2) % STEPS)
                above = [pltpu.roll(b, 1, 0) for b in before] if k == 0 else before
                below = [pltpu.roll(f, BLOCKS - 1, 0) for f in follow] if k + 2 == STEPS else follow
                middle = [jnp.minimum(h, a) for h, a in zip(here, after)]
                one = [jnp.maximum(jnp.minimum(a, m), mask[k, j]) for j, (a, m) in enumerate(zip(above, middle))]
                two = [jnp.maximum(jnp.minimum(m, b), mask[k + 1, j]) for j, (m, b) in enumerate(zip(middle, below))]
                for j in range(LSTEPS):
                    state[k, j] = one[j]
                    state[k + 1, j] = two[j]
                turn(k, one[0], one[-1])
                turn(k + 1, two[0], two[-1])
                before, here = after, follow
        return carry

    lax.fori_loop(0, SWEEPS // UNROLL, sweeps, 0)

    for k in range(STEPS):
        for j in range(LSTEPS):
            flat[j, pl.ds(k, BLOCKS, stride=STEPS), :] = state[k, j].astype(jnp.float32)
    for g in range(ROWS // 8):
        at = slice(8 * g, 8 * g + 8)
        values = [flat[j, at] for j in range(LSTEPS)]
        for t in range(4):
            place = lane + LANES * t
            lanes = place // LSTEPS
            step = place - lanes * LSTEPS
            value = jnp.take_along_axis(values[0], lanes, axis=1)
            for j in range(1, LSTEPS):
                value = jnp.where(step == j, jnp.take_along_axis(values[j], lanes, axis=1), value)
            out[at, LANES * t : LANES * t + LANES] = jnp.where(
                value >= EDGE, 0.0, jnp.log2(value) * (1 / SCALE) + SHIFT / SCALE
            )


def per_device(foreground, seed_keys):
    f32 = jnp.float32
    whole = pl.BlockSpec(memory_space=pltpu.VMEM)
    ext, sides, corners = pl.pallas_call(
        exchange_kernel,
        out_shape=[
            jax.ShapeDtypeStruct((WIDE, COLS), f32),
            jax.ShapeDtypeStruct((2, ROWS // 2, LANES), f32),
            jax.ShapeDtypeStruct((4, SWEEPS, LANES), f32),
        ],
        in_specs=[pl.BlockSpec(memory_space=pltpu.HBM)] * 2,
        out_specs=[whole] * 3,
        scratch_shapes=[
            pltpu.VMEM((ROWS, COLS), jnp.int32),
            pltpu.VMEM((ROWS, COLS), f32),
            pltpu.VMEM((2, ROWS // 2, LANES), f32),
            pltpu.SemaphoreType.DMA((2,)),
            pltpu.SemaphoreType.DMA((8,)),
            pltpu.SemaphoreType.DMA((8,)),
        ],
        compiler_params=pltpu.CompilerParams(
            collective_id=0, has_side_effects=True, vmem_limit_bytes=16 * 2**20
        ),
        name="exchange",
    )(foreground, seed_keys)
    bf16 = jnp.bfloat16
    return pl.pallas_call(
        sweep_kernel,
        out_shape=jax.ShapeDtypeStruct((ROWS, COLS), f32),
        in_specs=[whole] * 3,
        out_specs=whole,
        scratch_shapes=[
            pltpu.VMEM((LSTEPS, WIDE, LANES), f32),
            pltpu.VMEM((STEPS, LSTEPS, BLOCKS, LANES), bf16),
            pltpu.VMEM((STEPS, LSTEPS, BLOCKS, LANES), bf16),
            pltpu.VMEM((STEPS, 2, BLOCKS, LANES), bf16),
        ],
        compiler_params=pltpu.CompilerParams(vmem_limit_bytes=16 * 2**20),
        name="sweeps",
    )(ext, sides, corners)


def solution(mesh):
    placed = (P("row", "col"), P("row", "col"))
    return jax.shard_map(
        per_device, mesh=mesh, in_specs=placed, out_specs=P("row", "col"), check_vma=False
    )
```

```python
import functools

import jax
import jax.numpy as jnp
from jax import lax
from jax.experimental import pallas as pl
from jax.experimental.pallas import tpu as pltpu
from jax.sharding import PartitionSpec as P

SWEEPS = 48
SCALE = 240.0
SHIFT = 360.0
BIG = 2.0**126
EDGE = 2.0**125
LANES = 128
HALF = 64
ROWS = 256
COLS = 512
WIDE = ROWS + 2 * SWEEPS
BLOCKS = 16
STEPS = WIDE // BLOCKS
LSTEPS = 5
UNROLL = 12
DIRECTIONS = ((-1, -1), (-1, 1), (1, -1), (1, 1), (0, -1), (0, 1), (-1, 0), (1, 0))


def exchange_kernel(fg_hbm, key_hbm, ext, sides, corners, fg, key, packed, load_sem, send_sem, recv_sem):
    row, col = lax.axis_index("row"), lax.axis_index("col")
    rows, cols = lax.axis_size("row"), lax.axis_size("col")
    loads = [
        pltpu.make_async_copy(fg_hbm, fg, load_sem.at[0]),
        pltpu.make_async_copy(key_hbm, key, load_sem.at[1]),
    ]
    for load in loads:
        load.start()

    def present(dr, dc):
        r, c = row + dr, col + dc
        return (r >= 0) & (r < rows) & (c >= 0) & (c < cols)

    barrier = pltpu.get_barrier_semaphore()
    for dr, dc in DIRECTIONS:

        @pl.when(present(dr, dc))
        def _():
            pl.semaphore_signal(
                barrier, inc=1, device_id=(row + dr, col + dc), device_id_type=pl.DeviceIdType.MESH
            )

    for load in loads:
        load.wait()
    for t in range(4):
        at = slice(LANES * t, LANES * t + LANES)
        ext[t, :ROWS] = jnp.where(fg[:, at] == 1, jnp.exp2(key[:, at] * SCALE - SHIFT), BIG)
    low = lax.broadcasted_iota(jnp.int32, (ROWS // 2, LANES), 1) < HALF
    top, bottom = slice(0, ROWS // 2), slice(ROWS // 2, ROWS)
    packed[0] = jnp.where(low, ext[0, top], pltpu.roll(ext[0, bottom], HALF, 1))
    packed[1] = jnp.where(low, pltpu.roll(ext[3, bottom], HALF, 1), ext[3, top])

    heights = {-1: pl.ds(0, SWEEPS), 1: pl.ds(ROWS - SWEEPS, SWEEPS)}
    tiles = {-1: 0, 1: 3}
    halos = {-1: pl.ds(ROWS, SWEEPS), 1: pl.ds(ROWS + SWEEPS, SWEEPS)}

    def ends(dr, dc):
        if dr == 0:
            at = 0 if dc < 0 else 1
            return packed.at[at], sides.at[at]
        if dc == 0:
            return ext.at[:, heights[dr]], ext.at[:, halos[dr]]
        return ext.at[tiles[dc], heights[dr]], corners.at[(1 + dr) + (1 + dc) // 2]

    copies = []
    for i, (dr, dc) in enumerate(DIRECTIONS):
        src, dst = ends(dr, dc)
        copies.append(
            pltpu.make_async_remote_copy(
                src_ref=src,
                dst_ref=dst,
                send_sem=send_sem.at[i],
                recv_sem=recv_sem.at[i],
                device_id=(row + dr, col + dc),
                device_id_type=pl.DeviceIdType.MESH,
            )
        )
    count = jnp.int32(0)
    for dr, dc in DIRECTIONS:
        count += jnp.where(present(dr, dc), 1, 0)
    pl.semaphore_wait(barrier, count)
    for (dr, dc), copy in zip(DIRECTIONS, copies):
        pl.when(present(dr, dc))(copy.start)
    for (dr, dc), copy in zip(DIRECTIONS, copies):

        @pl.when(jnp.logical_not(present(-dr, -dc)))
        def _():
            dst = ends(dr, dc)[1]
            dst[...] = jnp.full(dst.shape, BIG, jnp.float32)

    for (dr, dc), copy in zip(DIRECTIONS, copies):
        pl.when(present(-dr, -dc))(copy.wait_recv)
    for (dr, dc), copy in zip(DIRECTIONS, copies):
        pl.when(present(dr, dc))(copy.wait_send)


def sweep_kernel(ext, sides, corners, out, side, result, sem):
    lane = lax.broadcasted_iota(jnp.int32, (8, LANES), 1)
    low = lane < HALF
    half = ROWS // 2
    for g in range(WIDE // 8):
        start = 8 * g
        if start < half:
            rows = slice(start, start + 8)
            value = jnp.where(low, sides[0, rows], sides[1, rows])
        elif start < ROWS:
            rows = slice(start - half, start - half + 8)
            value = pltpu.roll(jnp.where(low, sides[1, rows], sides[0, rows]), HALF, 1)
        elif start < ROWS + SWEEPS:
            rows = slice(start - ROWS, start - ROWS + 8)
            value = jnp.where(low, corners[0, rows], corners[1, rows])
        else:
            rows = slice(start - ROWS - SWEEPS, start - ROWS - SWEEPS + 8)
            value = jnp.where(low, corners[2, rows], corners[3, rows])
        side[start : start + 8] = value

    bf16, f32 = jnp.bfloat16, jnp.float32
    big = jnp.full((BLOCKS, LANES), BIG, bf16)
    zero = jnp.zeros((BLOCKS, LANES), bf16)
    place = lax.broadcasted_iota(jnp.int32, (BLOCKS, LANES), 1)

    def pick(value, lanes):
        return jnp.take_along_axis(value.astype(f32), lanes, axis=1).astype(bf16)

    def turn(first, last):
        return pltpu.roll(last, 1, 1), pltpu.roll(first, LANES - 1, 1)

    raw = []
    for k in range(STEPS):
        rows = pl.ds(k, BLOCKS, stride=STEPS)
        raw.append([ext[t, rows, :].astype(bf16) for t in range(4)] + [side[rows, :].astype(bf16)])
    state = [[None] * LSTEPS for _ in range(STEPS)]
    for j in range(LSTEPS):
        lanes = (place * LSTEPS + j) & (LANES - 1)
        for k in range(STEPS):
            value = pick(raw[k][0], lanes)
            for t in range(1, LSTEPS):
                value = jnp.where(place < -(-(LANES * t - j) // LSTEPS), value, pick(raw[k][t], lanes))
            state[k][j] = value
    mask = [[jnp.where(v >= EDGE, big, zero) for v in values] for values in state]
    turned = [turn(values[0], values[-1]) for values in state]

    def across(a, t):
        p, q = jnp.minimum(a[0], a[1]), jnp.minimum(a[2], a[3])
        return [
            jnp.minimum(t[0], p),
            jnp.minimum(p, a[2]),
            jnp.minimum(a[1], q),
            jnp.minimum(q, a[4]),
            jnp.minimum(jnp.minimum(a[3], a[4]), t[1]),
        ]

    def sweeps(i, carry):
        state, turned = carry
        state, turned = list(state), list(turned)
        for u in range(UNROLL):
            begin = 2 * u % STEPS
            before = across(state[(begin - 1) % STEPS], turned[(begin - 1) % STEPS])
            here = begin_row = across(state[begin], turned[begin])
            for pair in range(STEPS // 2):
                k = (begin + 2 * pair) % STEPS
                n = (k + 2) % STEPS
                after = across(state[k + 1], turned[k + 1])
                follow = begin_row if pair == STEPS // 2 - 1 else across(state[n], turned[n])
                above = [pltpu.roll(b, 1, 0) for b in before] if k == 0 else before
                below = [pltpu.roll(f, BLOCKS - 1, 0) for f in follow] if k + 2 == STEPS else follow
                middle = [jnp.minimum(h, a) for h, a in zip(here, after)]
                state[k] = [jnp.maximum(jnp.minimum(a, m), c) for a, m, c in zip(above, middle, mask[k])]
                state[k + 1] = [jnp.maximum(jnp.minimum(m, b), c) for m, b, c in zip(middle, below, mask[k + 1])]
                turned[k] = turn(state[k][0], state[k][-1])
                turned[k + 1] = turn(state[k + 1][0], state[k + 1][-1])
                before, here = after, follow
        return state, turned

    state, turned = lax.fori_loop(0, SWEEPS // UNROLL, sweeps, (state, turned))

    stores = []
    for t in range(4):
        at = place + LANES * t
        lanes = at // LSTEPS
        step = at - lanes * LSTEPS
        for k in range(STEPS):
            value = pick(state[k][0], lanes)
            for j in range(1, LSTEPS):
                value = jnp.where(step == j, pick(state[k][j], lanes), value)
            value = value.astype(f32)
            value = jnp.where(value >= EDGE, 0.0, jnp.log2(value) * (1 / SCALE) + SHIFT / SCALE)
            more = (ROWS - 1 - k) // STEPS + 1 - 8
            result[t, pl.ds(k, 8, stride=STEPS), :] = value[:8]
            result[t, pl.ds(k + 8 * STEPS, more, stride=STEPS), :] = value[8 : 8 + more]
        stores.append(pltpu.make_async_copy(result.at[t], out.at[:, pl.ds(LANES * t, LANES)], sem.at[t]))
        stores[-1].start()
    for store in stores:
        store.wait()


def per_device(foreground, seed_keys):
    f32 = jnp.float32
    whole = pl.BlockSpec(memory_space=pltpu.VMEM)
    ext, sides, corners = pl.pallas_call(
        exchange_kernel,
        out_shape=[
            jax.ShapeDtypeStruct((4, WIDE, LANES), f32),
            jax.ShapeDtypeStruct((2, ROWS // 2, LANES), f32),
            jax.ShapeDtypeStruct((4, SWEEPS, LANES), f32),
        ],
        in_specs=[pl.BlockSpec(memory_space=pltpu.HBM)] * 2,
        out_specs=[whole] * 3,
        scratch_shapes=[
            pltpu.VMEM((ROWS, COLS), jnp.int32),
            pltpu.VMEM((ROWS, COLS), f32),
            pltpu.VMEM((2, ROWS // 2, LANES), f32),
            pltpu.SemaphoreType.DMA((2,)),
            pltpu.SemaphoreType.DMA((8,)),
            pltpu.SemaphoreType.DMA((8,)),
        ],
        compiler_params=pltpu.CompilerParams(
            collective_id=0, has_side_effects=True, vmem_limit_bytes=16 * 2**20
        ),
        name="exchange",
    )(pltpu.with_memory_space_constraint(foreground, pltpu.HBM), pltpu.with_memory_space_constraint(seed_keys, pltpu.HBM))
    return pl.pallas_call(
        sweep_kernel,
        out_shape=jax.ShapeDtypeStruct((ROWS, COLS), f32),
        in_specs=[whole] * 3,
        out_specs=pl.BlockSpec(memory_space=pltpu.HBM),
        scratch_shapes=[
            pltpu.VMEM((WIDE, LANES), f32),
            pltpu.VMEM((4, ROWS, LANES), f32),
            pltpu.SemaphoreType.DMA((4,)),
        ],
        compiler_params=pltpu.CompilerParams(vmem_limit_bytes=16 * 2**20),
        name="sweeps",
    )(ext, sides, corners)


def solution(mesh):
    placed = (P("row", "col"), P("row", "col"))
    return jax.shard_map(
        per_device, mesh=mesh, in_specs=placed, out_specs=P("row", "col"), check_vma=False
    )
```

```python
import jax
import jax.numpy as jnp
from jax import lax
from jax.experimental import pallas as pl
from jax.experimental.pallas import tpu as pltpu
from jax.sharding import PartitionSpec as P

SWEEPS = 48
SCALE = 240.0
SHIFT = 360.0
BIG = 2.0**126
EDGE = 2.0**125
LANES = 128
HALF = 64
ROWS = 256
TILES = 4
WIDE = ROWS + 2 * SWEEPS
PART = SWEEPS // 2
BLOCKS = 16
STEPS = WIDE // BLOCKS
LSTEPS = 5
UNROLL = 24
DIRECTIONS = ((-1, -1), (-1, 1), (1, -1), (1, 1), (0, -1), (0, 1), (-1, 0), (1, 0))


def exchange_kernel(fg_hbm, key_hbm, ext, sides, corners, fg, key, columns, packed, load_sem, send_sem, recv_sem):
    row, col = lax.axis_index("row"), lax.axis_index("col")
    rows, cols = lax.axis_size("row"), lax.axis_size("col")
    loads = {}
    for t in (0, 3, 1, 2):
        tile = pl.ds(LANES * t, LANES)
        loads[t] = (
            pltpu.make_async_copy(fg_hbm.at[:, tile], fg.at[t], load_sem.at[0, t]),
            pltpu.make_async_copy(key_hbm.at[:, tile], key.at[t], load_sem.at[1, t]),
        )
        for load in loads[t]:
            load.start()

    def present(dr, dc):
        r, c = row + dr, col + dc
        return (r >= 0) & (r < rows) & (c >= 0) & (c < cols)

    barrier = pltpu.get_barrier_semaphore()
    count = jnp.int32(0)
    for dr, dc in DIRECTIONS:
        count += jnp.where(present(dr, dc), 1, 0)

        @pl.when(present(dr, dc))
        def _():
            pl.semaphore_signal(
                barrier, inc=1, device_id=(row + dr, col + dc), device_id_type=pl.DeviceIdType.MESH
            )

    heights = {-1: pl.ds(0, SWEEPS), 1: pl.ds(ROWS - SWEEPS, SWEEPS)}
    halos = {-1: pl.ds(ROWS, SWEEPS), 1: pl.ds(ROWS + SWEEPS, SWEEPS)}
    bands = {-1: pl.ds(0, SWEEPS), 1: pl.ds(LANES - SWEEPS, SWEEPS)}

    def corner(dr, dc):
        return (1 + dr) + (1 + dc) // 2

    def ends(dr, dc):
        if dr == 0:
            return columns.at[(1 + dc) // 2], sides.at[bands[dc]]
        if dc == 0:
            return ext.at[:, heights[dr]], ext.at[:, halos[dr]]
        return packed.at[corner(dr, dc)], corners.at[corner(dr, dc)]

    copies = {}
    for i, (dr, dc) in enumerate(DIRECTIONS):
        src, dst = ends(dr, dc)
        copies[dr, dc] = pltpu.make_async_remote_copy(
            src_ref=src,
            dst_ref=dst,
            send_sem=send_sem.at[i],
            recv_sem=recv_sem.at[i],
            device_id=(row + dr, col + dc),
            device_id_type=pl.DeviceIdType.MESH,
        )

    def encode(t):
        for load in loads[t]:
            load.wait()
        ext[t, :ROWS] = jnp.where(fg[t] == 1, jnp.exp2(key[t] * SCALE - SHIFT), BIG)

    low = lax.broadcasted_iota(jnp.int32, (PART, LANES), 1) < HALF
    for t, dc in ((0, -1), (3, 1)):
        encode(t)
        for dr, start in ((-1, 0), (1, ROWS - SWEEPS)):
            first = ext[t, start : start + PART]
            second = pltpu.roll(ext[t, start + PART : start + SWEEPS], HALF, 1)
            packed[corner(dr, dc)] = jnp.where(low, first, second) if dc < 0 else jnp.where(low, second, first)
        turned = ext[t, :ROWS].T
        columns[(1 + dc) // 2] = turned[:SWEEPS] if dc < 0 else turned[LANES - SWEEPS :]

    pl.semaphore_wait(barrier, count)
    for dr, dc in DIRECTIONS[:6]:
        pl.when(present(dr, dc))(copies[dr, dc].start)
    for t in (1, 2):
        encode(t)
    for dr, dc in DIRECTIONS[6:]:
        pl.when(present(dr, dc))(copies[dr, dc].start)

    sides[SWEEPS : LANES - SWEEPS] = jnp.full((LANES - 2 * SWEEPS, ROWS), BIG, jnp.float32)
    for dr, dc in DIRECTIONS:

        @pl.when(jnp.logical_not(present(-dr, -dc)))
        def _():
            dst = ends(dr, dc)[1]
            dst[...] = jnp.full(dst.shape, BIG, jnp.float32)

    for dr, dc in DIRECTIONS:
        pl.when(present(-dr, -dc))(copies[dr, dc].wait_recv)
    for dr, dc in DIRECTIONS:
        pl.when(present(dr, dc))(copies[dr, dc].wait_send)


def sweep_kernel(ext, sides, corners, out, side, result, sem):
    bf16, f32 = jnp.bfloat16, jnp.float32
    side[:ROWS] = sides[...].T
    low = lax.broadcasted_iota(jnp.int32, (PART, LANES), 1) < HALF
    for start, right, left in ((ROWS, 0, 1), (ROWS + SWEEPS, 2, 3)):
        side[start : start + PART] = jnp.where(low, corners[right], corners[left])
        other = jnp.where(low, corners[left], corners[right])
        side[start + PART : start + SWEEPS] = pltpu.roll(other, HALF, 1)

    big = jnp.full((BLOCKS, LANES), BIG, bf16)
    zero = jnp.zeros((BLOCKS, LANES), bf16)
    lane = lax.broadcasted_iota(jnp.int32, (BLOCKS, LANES), 1)
    phase = lane % LSTEPS

    def pick(value, lanes):
        return jnp.take_along_axis(value.astype(f32), lanes, axis=1).astype(bf16)

    def turn(first, last):
        return pltpu.roll(last, 1, 1), pltpu.roll(first, LANES - 1, 1)

    is_phase = [phase == p for p in range(LSTEPS)]
    state = []
    for k in range(STEPS):
        rows = pl.ds(k, BLOCKS, stride=STEPS)
        tiles = [ext[t, rows, :].astype(bf16) for t in range(TILES)] + [side[rows, :].astype(bf16)]
        steps = []
        for j in range(LSTEPS):
            value = tiles[0]
            for t in range(1, LSTEPS):
                value = jnp.where(is_phase[(j - 3 * t) % LSTEPS], tiles[t], value)
            steps.append(pick(value, (lane * LSTEPS + j) & (LANES - 1)))
        state.append(steps)
    mask = [[jnp.where(v >= EDGE, big, zero) for v in values] for values in state]
    turned = [turn(values[0], values[-1]) for values in state]

    def across(a, t):
        p, q = jnp.minimum(a[0], a[1]), jnp.minimum(a[2], a[3])
        return [
            jnp.minimum(t[0], p),
            jnp.minimum(p, a[2]),
            jnp.minimum(a[1], q),
            jnp.minimum(q, a[4]),
            jnp.minimum(jnp.minimum(a[3], a[4]), t[1]),
        ]

    def sweeps(i, carry):
        state, turned = carry
        state, turned = list(state), list(turned)
        for u in range(UNROLL):
            begin = 2 * u % STEPS
            before = across(state[(begin - 1) % STEPS], turned[(begin - 1) % STEPS])
            here = begin_row = across(state[begin], turned[begin])
            for pair in range(STEPS // 2):
                k = (begin + 2 * pair) % STEPS
                n = (k + 2) % STEPS
                after = across(state[k + 1], turned[k + 1])
                follow = begin_row if pair == STEPS // 2 - 1 else across(state[n], turned[n])
                above = [pltpu.roll(b, 1, 0) for b in before] if k == 0 else before
                below = [pltpu.roll(f, BLOCKS - 1, 0) for f in follow] if k + 2 == STEPS else follow
                middle = [jnp.minimum(h, a) for h, a in zip(here, after)]
                state[k] = [jnp.maximum(jnp.minimum(a, m), c) for a, m, c in zip(above, middle, mask[k])]
                state[k + 1] = [jnp.maximum(jnp.minimum(m, b), c) for m, b, c in zip(middle, below, mask[k + 1])]
                turned[k] = turn(state[k][0], state[k][-1])
                turned[k + 1] = turn(state[k + 1][0], state[k + 1][-1])
                before, here = after, follow
        return state, turned

    state, turned = lax.fori_loop(0, SWEEPS // UNROLL, sweeps, (state, turned))

    for k in range(STEPS):
        steps = []
        for j in range(LSTEPS):
            tile = (2 * (j - phase)) % LSTEPS
            steps.append(pick(state[k][j], (LANES * tile + lane) // LSTEPS))
        more = (ROWS - 1 - k) // STEPS + 1 - 8
        for t in range(TILES):
            value = steps[0]
            for j in range(1, LSTEPS):
                value = jnp.where(is_phase[(j - 3 * t) % LSTEPS], steps[j], value)
            value = value.astype(f32)
            value = jnp.where(value >= EDGE, 0.0, jnp.log2(value) * (1 / SCALE) + SHIFT / SCALE)
            result[t, pl.ds(k, 8, stride=STEPS), :] = value[:8]
            result[t, pl.ds(k + 8 * STEPS, more, stride=STEPS), :] = value[8 : 8 + more]
    stores = []
    for t in range(TILES):
        stores.append(pltpu.make_async_copy(result.at[t], out.at[:, pl.ds(LANES * t, LANES)], sem.at[t]))
        stores[-1].start()
    for store in stores:
        store.wait()


def per_device(foreground, seed_keys):
    f32 = jnp.float32
    whole = pl.BlockSpec(memory_space=pltpu.VMEM)
    hbm = pl.BlockSpec(memory_space=pltpu.HBM)
    ext, sides, corners = pl.pallas_call(
        exchange_kernel,
        out_shape=[
            jax.ShapeDtypeStruct((TILES, WIDE, LANES), f32),
            jax.ShapeDtypeStruct((LANES, ROWS), f32),
            jax.ShapeDtypeStruct((4, PART, LANES), f32),
        ],
        in_specs=[hbm] * 2,
        out_specs=[whole] * 3,
        scratch_shapes=[
            pltpu.VMEM((TILES, ROWS, LANES), jnp.int32),
            pltpu.VMEM((TILES, ROWS, LANES), f32),
            pltpu.VMEM((2, SWEEPS, ROWS), f32),
            pltpu.VMEM((4, PART, LANES), f32),
            pltpu.SemaphoreType.DMA((2, TILES)),
            pltpu.SemaphoreType.DMA((8,)),
            pltpu.SemaphoreType.DMA((8,)),
        ],
        compiler_params=pltpu.CompilerParams(
            collective_id=0, has_side_effects=True, vmem_limit_bytes=16 * 2**20
        ),
        name="exchange",
    )(
        pltpu.with_memory_space_constraint(foreground, pltpu.HBM),
        pltpu.with_memory_space_constraint(seed_keys, pltpu.HBM),
    )
    return pl.pallas_call(
        sweep_kernel,
        out_shape=jax.ShapeDtypeStruct((ROWS, TILES * LANES), f32),
        in_specs=[whole] * 3,
        out_specs=hbm,
        scratch_shapes=[
            pltpu.VMEM((WIDE, LANES), f32),
            pltpu.VMEM((TILES, ROWS, LANES), f32),
            pltpu.SemaphoreType.DMA((TILES,)),
        ],
        compiler_params=pltpu.CompilerParams(vmem_limit_bytes=16 * 2**20),
        name="sweeps",
    )(ext, sides, corners)


def solution(mesh):
    placed = (P("row", "col"), P("row", "col"))
    return jax.shard_map(
        per_device, mesh=mesh, in_specs=placed, out_specs=P("row", "col"), check_vma=False
    )
```

```python
import jax
import jax.numpy as jnp
from jax import lax
from jax.experimental import pallas as pl
from jax.experimental.pallas import tpu as pltpu
from jax.sharding import PartitionSpec as P

SWEEPS = 48
SCALE = 240.0
SHIFT = 360.0
BIG = 2.0**126
EDGE = 2.0**125
LANES = 128
HALF = 64
ROWS = 256
TILES = 4
WIDE = ROWS + 2 * SWEEPS
PART = SWEEPS // 2
BLOCKS = 16
STEPS = WIDE // BLOCKS
LSTEPS = 5
UNROLL = 24
DIRECTIONS = ((-1, -1), (-1, 1), (1, -1), (1, 1), (0, -1), (0, 1), (-1, 0), (1, 0))


def exchange_kernel(fg_hbm, key_hbm, ext, sides, corners, fg, key, columns, packed, load_sem, send_sem, recv_sem):
    row, col = lax.axis_index("row"), lax.axis_index("col")
    rows, cols = lax.axis_size("row"), lax.axis_size("col")
    loads = {}
    for t in (0, 3, 1, 2):
        tile = pl.ds(LANES * t, LANES)
        loads[t] = (
            pltpu.make_async_copy(fg_hbm.at[:, tile], fg.at[t], load_sem.at[0, t]),
            pltpu.make_async_copy(key_hbm.at[:, tile], key.at[t], load_sem.at[1, t]),
        )
        for load in loads[t]:
            load.start()

    def present(dr, dc):
        r, c = row + dr, col + dc
        return (r >= 0) & (r < rows) & (c >= 0) & (c < cols)

    barrier = pltpu.get_barrier_semaphore()
    count = jnp.int32(0)
    for dr, dc in DIRECTIONS:
        count += jnp.where(present(dr, dc), 1, 0)

        @pl.when(present(dr, dc))
        def _():
            pl.semaphore_signal(
                barrier, inc=1, device_id=(row + dr, col + dc), device_id_type=pl.DeviceIdType.MESH
            )

    heights = {-1: pl.ds(0, SWEEPS), 1: pl.ds(ROWS - SWEEPS, SWEEPS)}
    halos = {-1: pl.ds(ROWS, SWEEPS), 1: pl.ds(ROWS + SWEEPS, SWEEPS)}
    bands = {-1: pl.ds(0, SWEEPS), 1: pl.ds(LANES - SWEEPS, SWEEPS)}

    def corner(dr, dc):
        return (1 + dr) + (1 + dc) // 2

    def ends(dr, dc):
        if dr == 0:
            return columns.at[(1 + dc) // 2], sides.at[bands[dc]]
        if dc == 0:
            return ext.at[:, heights[dr]], ext.at[:, halos[dr]]
        return packed.at[corner(dr, dc)], corners.at[corner(dr, dc)]

    copies = {}
    for i, (dr, dc) in enumerate(DIRECTIONS):
        src, dst = ends(dr, dc)
        copies[dr, dc] = pltpu.make_async_remote_copy(
            src_ref=src,
            dst_ref=dst,
            send_sem=send_sem.at[i],
            recv_sem=recv_sem.at[i],
            device_id=(row + dr, col + dc),
            device_id_type=pl.DeviceIdType.MESH,
        )

    def encode(t):
        for load in loads[t]:
            load.wait()
        ext[t, :ROWS] = jnp.where(fg[t] == 1, jnp.exp2(key[t] * SCALE - SHIFT), BIG)

    low = lax.broadcasted_iota(jnp.int32, (PART, LANES), 1) < HALF
    for t, dc in ((0, -1), (3, 1)):
        encode(t)
        for dr, start in ((-1, 0), (1, ROWS - SWEEPS)):
            first = ext[t, start : start + PART]
            second = pltpu.roll(ext[t, start + PART : start + SWEEPS], HALF, 1)
            packed[corner(dr, dc)] = jnp.where(low, first, second) if dc < 0 else jnp.where(low, second, first)
        turned = ext[t, :ROWS].T
        columns[(1 + dc) // 2] = turned[:SWEEPS] if dc < 0 else turned[LANES - SWEEPS :]

    pl.semaphore_wait(barrier, count)
    early = row % 2 == 0
    for dr, dc in DIRECTIONS[:4]:
        pl.when(present(dr, dc) & (early if dr > 0 else jnp.logical_not(early)))(copies[dr, dc].start)
    for dr, dc in DIRECTIONS[4:6]:
        pl.when(present(dr, dc))(copies[dr, dc].start)
    for dr, dc in DIRECTIONS[:4]:
        pl.when(present(dr, dc) & (jnp.logical_not(early) if dr > 0 else early))(copies[dr, dc].start)
    for t in (1, 2):
        encode(t)
    for dr, dc in DIRECTIONS[6:]:
        pl.when(present(dr, dc))(copies[dr, dc].start)

    sides[SWEEPS : LANES - SWEEPS] = jnp.full((LANES - 2 * SWEEPS, ROWS), BIG, jnp.float32)
    for dr, dc in DIRECTIONS:

        @pl.when(jnp.logical_not(present(-dr, -dc)))
        def _():
            dst = ends(dr, dc)[1]
            dst[...] = jnp.full(dst.shape, BIG, jnp.float32)

    for dr, dc in DIRECTIONS:
        pl.when(present(-dr, -dc))(copies[dr, dc].wait_recv)
    for dr, dc in DIRECTIONS:
        pl.when(present(dr, dc))(copies[dr, dc].wait_send)


def sweep_kernel(ext, sides, corners, out, side, result, sem):
    bf16, f32 = jnp.bfloat16, jnp.float32
    side[:ROWS] = sides[...].T
    low = lax.broadcasted_iota(jnp.int32, (PART, LANES), 1) < HALF
    for start, right, left in ((ROWS, 0, 1), (ROWS + SWEEPS, 2, 3)):
        side[start : start + PART] = jnp.where(low, corners[right], corners[left])
        other = jnp.where(low, corners[left], corners[right])
        side[start + PART : start + SWEEPS] = pltpu.roll(other, HALF, 1)

    big = jnp.full((BLOCKS, LANES), BIG, bf16)
    zero = jnp.zeros((BLOCKS, LANES), bf16)
    lane = lax.broadcasted_iota(jnp.int32, (BLOCKS, LANES), 1)
    phase = lane % LSTEPS

    def pick(value, lanes):
        return jnp.take_along_axis(value.astype(f32), lanes, axis=1).astype(bf16)

    def turn(first, last):
        return pltpu.roll(last, 1, 1), pltpu.roll(first, LANES - 1, 1)

    is_phase = [phase == p for p in range(LSTEPS)]
    tiles = []
    for k in range(STEPS):
        rows = pl.ds(k, BLOCKS, stride=STEPS)
        tiles.append([ext[t, rows, :].astype(bf16) for t in range(TILES)] + [side[rows, :].astype(bf16)])
    state = [[None] * LSTEPS for _ in range(STEPS)]
    turned = [[None] * 2 for _ in range(STEPS)]
    for j in (4, 0, 1, 2, 3):
        for k in range(STEPS):
            value = tiles[k][0]
            for t in range(1, LSTEPS):
                value = jnp.where(is_phase[(j - 3 * t) % LSTEPS], tiles[k][t], value)
            state[k][j] = pick(value, (lane * LSTEPS + j) & (LANES - 1))
            if j == 4:
                turned[k][0] = pltpu.roll(state[k][j], 1, 1)
            if j == 0:
                turned[k][1] = pltpu.roll(state[k][j], LANES - 1, 1)
    mask = [[jnp.where(v >= EDGE, big, zero) for v in values] for values in state]

    def across(a, t):
        p, q = jnp.minimum(a[0], a[1]), jnp.minimum(a[2], a[3])
        return [
            jnp.minimum(t[0], p),
            jnp.minimum(p, a[2]),
            jnp.minimum(a[1], q),
            jnp.minimum(q, a[4]),
            jnp.minimum(jnp.minimum(a[3], a[4]), t[1]),
        ]

    def sweeps(i, carry):
        state, turned = carry
        state, turned = list(state), list(turned)
        for u in range(UNROLL):
            begin = 2 * u % STEPS
            before = across(state[(begin - 1) % STEPS], turned[(begin - 1) % STEPS])
            here = begin_row = across(state[begin], turned[begin])
            for pair in range(STEPS // 2):
                k = (begin + 2 * pair) % STEPS
                n = (k + 2) % STEPS
                after = across(state[k + 1], turned[k + 1])
                follow = begin_row if pair == STEPS // 2 - 1 else across(state[n], turned[n])
                above = [pltpu.roll(b, 1, 0) for b in before] if k == 0 else before
                below = [pltpu.roll(f, BLOCKS - 1, 0) for f in follow] if k + 2 == STEPS else follow
                middle = [jnp.minimum(h, a) for h, a in zip(here, after)]
                state[k] = [jnp.maximum(jnp.minimum(a, m), c) for a, m, c in zip(above, middle, mask[k])]
                state[k + 1] = [jnp.maximum(jnp.minimum(m, b), c) for m, b, c in zip(middle, below, mask[k + 1])]
                turned[k] = list(turn(state[k][0], state[k][-1]))
                turned[k + 1] = list(turn(state[k + 1][0], state[k + 1][-1]))
                before, here = after, follow
        return state, turned

    state, turned = lax.fori_loop(0, SWEEPS // UNROLL, sweeps, (state, turned))

    steps = []
    for j in range(LSTEPS):
        tile = (2 * (j - phase)) % LSTEPS
        lanes = (LANES * tile + lane) // LSTEPS
        steps.append([pick(state[k][j], lanes) for k in range(STEPS)])
    stores = []
    for t in range(TILES):
        for k in range(STEPS):
            value = steps[0][k]
            for j in range(1, LSTEPS):
                value = jnp.where(is_phase[(j - 3 * t) % LSTEPS], steps[j][k], value)
            value = value.astype(f32)
            value = jnp.where(value >= EDGE, 0.0, jnp.log2(value) * (1 / SCALE) + SHIFT / SCALE)
            more = (ROWS - 1 - k) // STEPS + 1 - 8
            result[t, pl.ds(k, 8, stride=STEPS), :] = value[:8]
            result[t, pl.ds(k + 8 * STEPS, more, stride=STEPS), :] = value[8 : 8 + more]
        stores.append(pltpu.make_async_copy(result.at[t], out.at[:, pl.ds(LANES * t, LANES)], sem.at[t]))
        stores[-1].start()
    for store in stores:
        store.wait()


def per_device(foreground, seed_keys):
    f32 = jnp.float32
    whole = pl.BlockSpec(memory_space=pltpu.VMEM)
    hbm = pl.BlockSpec(memory_space=pltpu.HBM)
    ext, sides, corners = pl.pallas_call(
        exchange_kernel,
        out_shape=[
            jax.ShapeDtypeStruct((TILES, WIDE, LANES), f32),
            jax.ShapeDtypeStruct((LANES, ROWS), f32),
            jax.ShapeDtypeStruct((4, PART, LANES), f32),
        ],
        in_specs=[hbm] * 2,
        out_specs=[whole] * 3,
        scratch_shapes=[
            pltpu.VMEM((TILES, ROWS, LANES), jnp.int32),
            pltpu.VMEM((TILES, ROWS, LANES), f32),
            pltpu.VMEM((2, SWEEPS, ROWS), f32),
            pltpu.VMEM((4, PART, LANES), f32),
            pltpu.SemaphoreType.DMA((2, TILES)),
            pltpu.SemaphoreType.DMA((8,)),
            pltpu.SemaphoreType.DMA((8,)),
        ],
        compiler_params=pltpu.CompilerParams(
            collective_id=0, has_side_effects=True, vmem_limit_bytes=16 * 2**20
        ),
        name="exchange",
    )(
        pltpu.with_memory_space_constraint(foreground, pltpu.HBM),
        pltpu.with_memory_space_constraint(seed_keys, pltpu.HBM),
    )
    return pl.pallas_call(
        sweep_kernel,
        out_shape=jax.ShapeDtypeStruct((ROWS, TILES * LANES), f32),
        in_specs=[whole] * 3,
        out_specs=hbm,
        scratch_shapes=[
            pltpu.VMEM((WIDE, LANES), f32),
            pltpu.VMEM((TILES, ROWS, LANES), f32),
            pltpu.SemaphoreType.DMA((TILES,)),
        ],
        compiler_params=pltpu.CompilerParams(vmem_limit_bytes=16 * 2**20),
        name="sweeps",
    )(ext, sides, corners)


def solution(mesh):
    placed = (P("row", "col"), P("row", "col"))
    return jax.shard_map(
        per_device, mesh=mesh, in_specs=placed, out_specs=P("row", "col"), check_vma=False
    )
```

```python
import jax
import jax.numpy as jnp
from jax import lax
from jax.experimental import pallas as pl
from jax.experimental.pallas import tpu as pltpu
from jax.sharding import PartitionSpec as P

SWEEPS = 48
SCALE = 240.0
SHIFT = 360.0
BIG = 2.0**126
EDGE = 2.0**125
LANES = 128
HALF = 64
ROWS = 256
TILES = 4
WIDE = ROWS + 2 * SWEEPS
PART = SWEEPS // 2
BLOCKS = 16
STEPS = WIDE // BLOCKS
LSTEPS = 5
DIRECTIONS = ((-1, -1), (-1, 1), (1, -1), (1, 1), (0, -1), (0, 1), (-1, 0), (1, 0))


def exchange_kernel(fg_hbm, key_hbm, ext, sides, corners, fg, key, columns, packed, load_sem, send_sem, recv_sem):
    row, col = lax.axis_index("row"), lax.axis_index("col")
    rows, cols = lax.axis_size("row"), lax.axis_size("col")
    loads = {}
    for t in (0, 3, 1, 2):
        tile = pl.ds(LANES * t, LANES)
        loads[t] = (
            pltpu.make_async_copy(fg_hbm.at[:, tile], fg.at[t], load_sem.at[0, t]),
            pltpu.make_async_copy(key_hbm.at[:, tile], key.at[t], load_sem.at[1, t]),
        )
        for load in loads[t]:
            load.start()

    def present(dr, dc):
        r, c = row + dr, col + dc
        return (r >= 0) & (r < rows) & (c >= 0) & (c < cols)

    barrier = pltpu.get_barrier_semaphore()
    count = jnp.int32(0)
    for dr, dc in DIRECTIONS:
        count += jnp.where(present(dr, dc), 1, 0)

        @pl.when(present(dr, dc))
        def _():
            pl.semaphore_signal(
                barrier, inc=1, device_id=(row + dr, col + dc), device_id_type=pl.DeviceIdType.MESH
            )

    heights = {-1: pl.ds(0, SWEEPS), 1: pl.ds(ROWS - SWEEPS, SWEEPS)}
    halos = {-1: pl.ds(ROWS, SWEEPS), 1: pl.ds(ROWS + SWEEPS, SWEEPS)}
    bands = {-1: pl.ds(0, SWEEPS), 1: pl.ds(LANES - SWEEPS, SWEEPS)}

    def corner(dr, dc):
        return (1 + dr) + (1 + dc) // 2

    def ends(dr, dc):
        if dr == 0:
            return columns.at[(1 + dc) // 2], sides.at[bands[dc]]
        if dc == 0:
            return ext.at[:, heights[dr]], ext.at[:, halos[dr]]
        return packed.at[corner(dr, dc)], corners.at[corner(dr, dc)]

    copies = {}
    for i, (dr, dc) in enumerate(DIRECTIONS):
        src, dst = ends(dr, dc)
        copies[dr, dc] = pltpu.make_async_remote_copy(
            src_ref=src,
            dst_ref=dst,
            send_sem=send_sem.at[i],
            recv_sem=recv_sem.at[i],
            device_id=(row + dr, col + dc),
            device_id_type=pl.DeviceIdType.MESH,
        )

    def encode(t):
        for load in loads[t]:
            load.wait()
        ext[t, :ROWS] = jnp.where(fg[t] == 1, jnp.exp2(key[t] * SCALE - SHIFT), BIG)

    low = lax.broadcasted_iota(jnp.int32, (PART, LANES), 1) < HALF
    for t, dc in ((0, -1), (3, 1)):
        encode(t)
        for dr, start in ((-1, 0), (1, ROWS - SWEEPS)):
            first = ext[t, start : start + PART]
            second = pltpu.roll(ext[t, start + PART : start + SWEEPS], HALF, 1)
            packed[corner(dr, dc)] = jnp.where(low, first, second) if dc < 0 else jnp.where(low, second, first)
        turned = ext[t, :ROWS].T
        columns[(1 + dc) // 2] = turned[:SWEEPS] if dc < 0 else turned[LANES - SWEEPS :]

    pl.semaphore_wait(barrier, count)
    early = row % 2 == 0
    for dr, dc in DIRECTIONS[:4]:
        pl.when(present(dr, dc) & (early if dr > 0 else jnp.logical_not(early)))(copies[dr, dc].start)
    for dr, dc in DIRECTIONS[4:6]:
        pl.when(present(dr, dc))(copies[dr, dc].start)
    for dr, dc in DIRECTIONS[:4]:
        pl.when(present(dr, dc) & (jnp.logical_not(early) if dr > 0 else early))(copies[dr, dc].start)
    for t in (1, 2):
        encode(t)
    for dr, dc in DIRECTIONS[6:]:
        pl.when(present(dr, dc))(copies[dr, dc].start)

    sides[SWEEPS : LANES - SWEEPS] = jnp.full((LANES - 2 * SWEEPS, ROWS), BIG, jnp.float32)
    for dr, dc in DIRECTIONS:

        @pl.when(jnp.logical_not(present(-dr, -dc)))
        def _():
            dst = ends(dr, dc)[1]
            dst[...] = jnp.full(dst.shape, BIG, jnp.float32)

    for dr, dc in DIRECTIONS:
        pl.when(present(-dr, -dc))(copies[dr, dc].wait_recv)
    for dr, dc in DIRECTIONS:
        pl.when(present(dr, dc))(copies[dr, dc].wait_send)


def sweep_kernel(ext, sides, corners, out, side, result, sem):
    bf16, f32 = jnp.bfloat16, jnp.float32
    side[:ROWS] = sides[...].T
    low = lax.broadcasted_iota(jnp.int32, (PART, LANES), 1) < HALF
    for start, right, left in ((ROWS, 0, 1), (ROWS + SWEEPS, 2, 3)):
        side[start : start + PART] = jnp.where(low, corners[right], corners[left])
        other = jnp.where(low, corners[left], corners[right])
        side[start + PART : start + SWEEPS] = pltpu.roll(other, HALF, 1)

    big = jnp.full((BLOCKS, LANES), BIG, bf16)
    zero = jnp.zeros((BLOCKS, LANES), bf16)
    lane = lax.broadcasted_iota(jnp.int32, (BLOCKS, LANES), 1)
    phase = lane % LSTEPS

    def pick(value, lanes):
        return jnp.take_along_axis(value.astype(f32), lanes, axis=1).astype(bf16)

    def turn(first, last):
        return pltpu.roll(last, 1, 1), pltpu.roll(first, LANES - 1, 1)

    is_phase = [phase == p for p in range(LSTEPS)]
    tiles = []
    for k in range(STEPS):
        rows = pl.ds(k, BLOCKS, stride=STEPS)
        tiles.append([ext[t, rows, :].astype(bf16) for t in range(TILES)] + [side[rows, :].astype(bf16)])
    state = [[None] * LSTEPS for _ in range(STEPS)]
    for j in range(LSTEPS):
        for k in range(STEPS):
            value = tiles[k][0]
            for t in range(1, LSTEPS):
                value = jnp.where(is_phase[(j - 3 * t) % LSTEPS], tiles[k][t], value)
            state[k][j] = pick(value, (lane * LSTEPS + j) & (LANES - 1))
    mask = [[jnp.where(v >= EDGE, big, zero) for v in values] for values in state]

    def across(a, t):
        p, q = jnp.minimum(a[0], a[1]), jnp.minimum(a[2], a[3])
        return [
            jnp.minimum(t[0], p),
            jnp.minimum(p, a[2]),
            jnp.minimum(a[1], q),
            jnp.minimum(q, a[4]),
            jnp.minimum(jnp.minimum(a[3], a[4]), t[1]),
        ]

    turned = [turn(values[0], values[-1]) for values in state]
    for _ in range(SWEEPS):
        before = across(state[-1], turned[-1])
        here = top = across(state[0], turned[0])
        for k in range(0, STEPS, 2):
            after = across(state[k + 1], turned[k + 1])
            follow = across(state[k + 2], turned[k + 2]) if k + 2 < STEPS else top
            above = before if k else [pltpu.roll(b, 1, 0) for b in before]
            below = follow if k + 2 < STEPS else [pltpu.roll(f, BLOCKS - 1, 0) for f in follow]
            middle = [jnp.minimum(h, a) for h, a in zip(here, after)]
            state[k] = [jnp.maximum(jnp.minimum(a, m), c) for a, m, c in zip(above, middle, mask[k])]
            state[k + 1] = [jnp.maximum(jnp.minimum(m, b), c) for m, b, c in zip(middle, below, mask[k + 1])]
            turned[k] = turn(state[k][0], state[k][-1])
            turned[k + 1] = turn(state[k + 1][0], state[k + 1][-1])
            before, here = after, follow

    lanes = [(LANES * ((2 * (j - phase)) % LSTEPS) + lane) // LSTEPS for j in range(LSTEPS)]
    stores = []
    for k in range(STEPS):
        steps = [pick(state[k][j], lanes[j]) for j in range(LSTEPS)]
        more = (ROWS - 1 - k) // STEPS + 1 - 8
        for t in range(TILES):
            value = steps[0]
            for j in range(1, LSTEPS):
                value = jnp.where(is_phase[(j - 3 * t) % LSTEPS], steps[j], value)
            value = value.astype(f32)
            value = jnp.where(value >= EDGE, 0.0, jnp.log2(value) * (1 / SCALE) + SHIFT / SCALE)
            result[t, pl.ds(k, 8, stride=STEPS), :] = value[:8]
            result[t, pl.ds(k + 8 * STEPS, more, stride=STEPS), :] = value[8 : 8 + more]
    for t in range(TILES):
        stores.append(pltpu.make_async_copy(result.at[t], out.at[:, pl.ds(LANES * t, LANES)], sem.at[t]))
        stores[-1].start()
    for store in stores:
        store.wait()


def per_device(foreground, seed_keys):
    f32 = jnp.float32
    whole = pl.BlockSpec(memory_space=pltpu.VMEM)
    hbm = pl.BlockSpec(memory_space=pltpu.HBM)
    ext, sides, corners = pl.pallas_call(
        exchange_kernel,
        out_shape=[
            jax.ShapeDtypeStruct((TILES, WIDE, LANES), f32),
            jax.ShapeDtypeStruct((LANES, ROWS), f32),
            jax.ShapeDtypeStruct((4, PART, LANES), f32),
        ],
        in_specs=[hbm] * 2,
        out_specs=[whole] * 3,
        scratch_shapes=[
            pltpu.VMEM((TILES, ROWS, LANES), jnp.int32),
            pltpu.VMEM((TILES, ROWS, LANES), f32),
            pltpu.VMEM((2, SWEEPS, ROWS), f32),
            pltpu.VMEM((4, PART, LANES), f32),
            pltpu.SemaphoreType.DMA((2, TILES)),
            pltpu.SemaphoreType.DMA((8,)),
            pltpu.SemaphoreType.DMA((8,)),
        ],
        compiler_params=pltpu.CompilerParams(
            collective_id=0, has_side_effects=True, vmem_limit_bytes=16 * 2**20
        ),
        name="exchange",
    )(
        pltpu.with_memory_space_constraint(foreground, pltpu.HBM),
        pltpu.with_memory_space_constraint(seed_keys, pltpu.HBM),
    )
    return pl.pallas_call(
        sweep_kernel,
        out_shape=jax.ShapeDtypeStruct((ROWS, TILES * LANES), f32),
        in_specs=[whole] * 3,
        out_specs=hbm,
        scratch_shapes=[
            pltpu.VMEM((WIDE, LANES), f32),
            pltpu.VMEM((TILES, ROWS, LANES), f32),
            pltpu.SemaphoreType.DMA((TILES,)),
        ],
        compiler_params=pltpu.CompilerParams(vmem_limit_bytes=16 * 2**20),
        name="sweeps",
    )(ext, sides, corners)


def solution(mesh):
    placed = (P("row", "col"), P("row", "col"))
    return jax.shard_map(
        per_device, mesh=mesh, in_specs=placed, out_specs=P("row", "col"), check_vma=False
    )
```

```python
import jax
import jax.numpy as jnp
from jax import lax
from jax.experimental import pallas as pl
from jax.experimental.pallas import tpu as pltpu
from jax.sharding import PartitionSpec as P

SWEEPS = 48
SCALE = 240.0
SHIFT = 360.0
BIG = 2.0**126
EDGE = 2.0**125
LANES = 128
HALF = 64
ROWS = 256
TILES = 4
WIDE = ROWS + 2 * SWEEPS
PART = SWEEPS // 2
BLOCKS = 16
STEPS = WIDE // BLOCKS
LSTEPS = 5
DIRECTIONS = ((-1, -1), (-1, 1), (1, -1), (1, 1), (0, -1), (0, 1), (-1, 0), (1, 0))


def exchange_kernel(
    fg_hbm, key_hbm, ext, side, sides, corners, fg, key, columns, packed, load_sem, send_sem, recv_sem
):
    row, col = lax.axis_index("row"), lax.axis_index("col")
    rows, cols = lax.axis_size("row"), lax.axis_size("col")
    loads = {}
    for t in (0, 3, 1, 2):
        tile = pl.ds(LANES * t, LANES)
        loads[t] = (
            pltpu.make_async_copy(fg_hbm.at[:, tile], fg.at[t], load_sem.at[0, t]),
            pltpu.make_async_copy(key_hbm.at[:, tile], key.at[t], load_sem.at[1, t]),
        )
        for load in loads[t]:
            load.start()

    def present(dr, dc):
        r, c = row + dr, col + dc
        return (r >= 0) & (r < rows) & (c >= 0) & (c < cols)

    barrier = pltpu.get_barrier_semaphore()
    count = jnp.int32(0)
    for dr, dc in DIRECTIONS:
        count += jnp.where(present(dr, dc), 1, 0)

        @pl.when(present(dr, dc))
        def _():
            pl.semaphore_signal(
                barrier, inc=1, device_id=(row + dr, col + dc), device_id_type=pl.DeviceIdType.MESH
            )

    heights = {-1: pl.ds(0, SWEEPS), 1: pl.ds(ROWS - SWEEPS, SWEEPS)}
    halos = {-1: pl.ds(ROWS, SWEEPS), 1: pl.ds(ROWS + SWEEPS, SWEEPS)}
    bands = {-1: pl.ds(0, SWEEPS), 1: pl.ds(LANES - SWEEPS, SWEEPS)}

    def corner(dr, dc):
        return (1 + dr) + (1 + dc) // 2

    def ends(dr, dc):
        if dr == 0:
            return columns.at[(1 + dc) // 2], sides.at[bands[dc]]
        if dc == 0:
            return ext.at[:, heights[dr]], ext.at[:, halos[dr]]
        return packed.at[corner(dr, dc)], corners.at[corner(dr, dc)]

    copies = {}
    for i, (dr, dc) in enumerate(DIRECTIONS):
        src, dst = ends(dr, dc)
        copies[dr, dc] = pltpu.make_async_remote_copy(
            src_ref=src,
            dst_ref=dst,
            send_sem=send_sem.at[i],
            recv_sem=recv_sem.at[i],
            device_id=(row + dr, col + dc),
            device_id_type=pl.DeviceIdType.MESH,
        )

    def encode(t):
        for load in loads[t]:
            load.wait()
        ext[t, :ROWS] = jnp.where(fg[t] == 1, jnp.exp2(key[t] * SCALE - SHIFT), BIG)

    low = lax.broadcasted_iota(jnp.int32, (PART, LANES), 1) < HALF
    for t, dc in ((0, -1), (3, 1)):
        encode(t)
        for dr, start in ((-1, 0), (1, ROWS - SWEEPS)):
            first = ext[t, start : start + PART]
            second = pltpu.roll(ext[t, start + PART : start + SWEEPS], HALF, 1)
            packed[corner(dr, dc)] = jnp.where(low, first, second) if dc < 0 else jnp.where(low, second, first)
        turned = ext[t, :ROWS].T
        columns[(1 + dc) // 2] = turned[:SWEEPS] if dc < 0 else turned[LANES - SWEEPS :]

    pl.semaphore_wait(barrier, count)
    early = row % 2 == 0
    for dr, dc in DIRECTIONS[:4]:
        pl.when(present(dr, dc) & (early if dr > 0 else jnp.logical_not(early)))(copies[dr, dc].start)
    for dr, dc in DIRECTIONS[4:6]:
        pl.when(present(dr, dc))(copies[dr, dc].start)
    for dr, dc in DIRECTIONS[:4]:
        pl.when(present(dr, dc) & (jnp.logical_not(early) if dr > 0 else early))(copies[dr, dc].start)
    for t in (1, 2):
        encode(t)
    for dr, dc in DIRECTIONS[6:]:
        pl.when(present(dr, dc))(copies[dr, dc].start)

    sides[SWEEPS : LANES - SWEEPS] = jnp.full((LANES - 2 * SWEEPS, ROWS), BIG, jnp.float32)
    for dr, dc in DIRECTIONS:

        @pl.when(jnp.logical_not(present(-dr, -dc)))
        def _():
            dst = ends(dr, dc)[1]
            dst[...] = jnp.full(dst.shape, BIG, jnp.float32)

    for dr, dc in DIRECTIONS[4:6]:
        pl.when(present(-dr, -dc))(copies[dr, dc].wait_recv)
    side[:ROWS] = sides[...].T
    for dr, dc in DIRECTIONS:
        pl.when(present(dr, dc))(copies[dr, dc].wait_send)
    for dr, dc in DIRECTIONS[6:] + DIRECTIONS[:4]:
        pl.when(present(-dr, -dc))(copies[dr, dc].wait_recv)
    for start, right, left in ((ROWS, 0, 1), (ROWS + SWEEPS, 2, 3)):
        side[start : start + PART] = jnp.where(low, corners[right], corners[left])
        other = jnp.where(low, corners[left], corners[right])
        side[start + PART : start + SWEEPS] = pltpu.roll(other, HALF, 1)


def sweep_kernel(ext, side, out, result, sem):
    bf16, f32 = jnp.bfloat16, jnp.float32
    big = jnp.full((BLOCKS, LANES), BIG, bf16)
    zero = jnp.zeros((BLOCKS, LANES), bf16)
    lane = lax.broadcasted_iota(jnp.int32, (BLOCKS, LANES), 1)
    phase = lane % LSTEPS

    def pick(value, lanes):
        return jnp.take_along_axis(value.astype(f32), lanes, axis=1).astype(bf16)

    def turn(first, last):
        return pltpu.roll(last, 1, 1), pltpu.roll(first, LANES - 1, 1)

    is_phase = [phase == p for p in range(LSTEPS)]
    tiles = []
    for k in range(STEPS):
        rows = pl.ds(k, BLOCKS, stride=STEPS)
        tiles.append([ext[t, rows, :].astype(bf16) for t in range(TILES)] + [side[rows, :].astype(bf16)])
    state = [[None] * LSTEPS for _ in range(STEPS)]
    for j in range(LSTEPS):
        for k in range(STEPS):
            value = tiles[k][0]
            for t in range(1, LSTEPS):
                value = jnp.where(is_phase[(j - 3 * t) % LSTEPS], tiles[k][t], value)
            state[k][j] = pick(value, (lane * LSTEPS + j) & (LANES - 1))
    mask = [[jnp.where(v >= EDGE, big, zero) for v in values] for values in state]

    def across(a, t):
        p, q = jnp.minimum(a[0], a[1]), jnp.minimum(a[2], a[3])
        return [
            jnp.minimum(t[0], p),
            jnp.minimum(p, a[2]),
            jnp.minimum(a[1], q),
            jnp.minimum(q, a[4]),
            jnp.minimum(jnp.minimum(a[3], a[4]), t[1]),
        ]

    turned = [turn(values[0], values[-1]) for values in state]
    for _ in range(SWEEPS):
        before = across(state[-1], turned[-1])
        here = top = across(state[0], turned[0])
        for k in range(0, STEPS, 2):
            after = across(state[k + 1], turned[k + 1])
            follow = across(state[k + 2], turned[k + 2]) if k + 2 < STEPS else top
            above = before if k else [pltpu.roll(b, 1, 0) for b in before]
            below = follow if k + 2 < STEPS else [pltpu.roll(f, BLOCKS - 1, 0) for f in follow]
            middle = [jnp.minimum(h, a) for h, a in zip(here, after)]
            state[k] = [jnp.maximum(jnp.minimum(a, m), c) for a, m, c in zip(above, middle, mask[k])]
            state[k + 1] = [jnp.maximum(jnp.minimum(m, b), c) for m, b, c in zip(middle, below, mask[k + 1])]
            turned[k] = turn(state[k][0], state[k][-1])
            turned[k + 1] = turn(state[k + 1][0], state[k + 1][-1])
            before, here = after, follow

    lanes = [(LANES * ((2 * (j - phase)) % LSTEPS) + lane) // LSTEPS for j in range(LSTEPS)]
    stores = []
    for k in range(STEPS):
        steps = [pick(state[k][j], lanes[j]) for j in range(LSTEPS)]
        more = (ROWS - 1 - k) // STEPS + 1 - 8
        for t in range(TILES):
            value = steps[0]
            for j in range(1, LSTEPS):
                value = jnp.where(is_phase[(j - 3 * t) % LSTEPS], steps[j], value)
            value = value.astype(f32)
            value = jnp.where(value >= EDGE, 0.0, jnp.log2(value) * (1 / SCALE) + SHIFT / SCALE)
            result[t, pl.ds(k, 8, stride=STEPS), :] = value[:8]
            result[t, pl.ds(k + 8 * STEPS, more, stride=STEPS), :] = value[8 : 8 + more]
    for t in range(TILES):
        stores.append(pltpu.make_async_copy(result.at[t], out.at[:, pl.ds(LANES * t, LANES)], sem.at[t]))
        stores[-1].start()
    for store in stores:
        store.wait()


def per_device(foreground, seed_keys):
    f32 = jnp.float32
    whole = pl.BlockSpec(memory_space=pltpu.VMEM)
    hbm = pl.BlockSpec(memory_space=pltpu.HBM)
    ext, side = pl.pallas_call(
        exchange_kernel,
        out_shape=[
            jax.ShapeDtypeStruct((TILES, WIDE, LANES), f32),
            jax.ShapeDtypeStruct((WIDE, LANES), f32),
        ],
        in_specs=[hbm] * 2,
        out_specs=[whole] * 2,
        scratch_shapes=[
            pltpu.VMEM((LANES, ROWS), f32),
            pltpu.VMEM((4, PART, LANES), f32),
            pltpu.VMEM((TILES, ROWS, LANES), jnp.int32),
            pltpu.VMEM((TILES, ROWS, LANES), f32),
            pltpu.VMEM((2, SWEEPS, ROWS), f32),
            pltpu.VMEM((4, PART, LANES), f32),
            pltpu.SemaphoreType.DMA((2, TILES)),
            pltpu.SemaphoreType.DMA((8,)),
            pltpu.SemaphoreType.DMA((8,)),
        ],
        compiler_params=pltpu.CompilerParams(
            collective_id=0, has_side_effects=True, vmem_limit_bytes=16 * 2**20
        ),
        name="exchange",
    )(
        pltpu.with_memory_space_constraint(foreground, pltpu.HBM),
        pltpu.with_memory_space_constraint(seed_keys, pltpu.HBM),
    )
    return pl.pallas_call(
        sweep_kernel,
        out_shape=jax.ShapeDtypeStruct((ROWS, TILES * LANES), f32),
        in_specs=[whole] * 2,
        out_specs=hbm,
        scratch_shapes=[
            pltpu.VMEM((TILES, ROWS, LANES), f32),
            pltpu.SemaphoreType.DMA((TILES,)),
        ],
        compiler_params=pltpu.CompilerParams(vmem_limit_bytes=16 * 2**20),
        name="sweeps",
    )(ext, side)


def solution(mesh):
    placed = (P("row", "col"), P("row", "col"))
    return jax.shard_map(
        per_device, mesh=mesh, in_specs=placed, out_specs=P("row", "col"), check_vma=False
    )
```

```python
import jax
import jax.numpy as jnp
from jax import lax
from jax.experimental import pallas as pl
from jax.experimental.pallas import tpu as pltpu
from jax.sharding import PartitionSpec as P

SWEEPS = 48
SCALE = 240.0
SHIFT = 360.0
BIG = 2.0**126
EDGE = 2.0**125
LANES = 128
HALF = 64
ROWS = 256
TILES = 4
WIDE = ROWS + 2 * SWEEPS
PART = SWEEPS // 2
BLOCKS = 16
STEPS = WIDE // BLOCKS
LSTEPS = 5
DIRECTIONS = ((-1, -1), (-1, 1), (1, -1), (1, 1), (0, -1), (0, 1), (-1, 0), (1, 0))


def exchange_kernel(
    fg_hbm, key_hbm, ext, side, sides, corners, fg, key, columns, packed, load_sem, send_sem, recv_sem
):
    row, col = lax.axis_index("row"), lax.axis_index("col")
    rows, cols = lax.axis_size("row"), lax.axis_size("col")
    def present(dr, dc):
        r, c = row + dr, col + dc
        return (r >= 0) & (r < rows) & (c >= 0) & (c < cols)

    barrier = pltpu.get_barrier_semaphore()
    count = jnp.int32(0)
    for dr, dc in DIRECTIONS:
        count += jnp.where(present(dr, dc), 1, 0)

        @pl.when(present(dr, dc))
        def _():
            pl.semaphore_signal(
                barrier, inc=1, device_id=(row + dr, col + dc), device_id_type=pl.DeviceIdType.MESH
            )

    loads = {}
    for t in (0, 3, 1, 2):
        tile = pl.ds(LANES * t, LANES)
        loads[t] = (
            pltpu.make_async_copy(fg_hbm.at[:, tile], fg.at[t], load_sem.at[0, t]),
            pltpu.make_async_copy(key_hbm.at[:, tile], key.at[t], load_sem.at[1, t]),
        )
        for load in loads[t]:
            load.start()

    heights = {-1: pl.ds(0, SWEEPS), 1: pl.ds(ROWS - SWEEPS, SWEEPS)}
    halos = {-1: pl.ds(ROWS, SWEEPS), 1: pl.ds(ROWS + SWEEPS, SWEEPS)}
    bands = {-1: pl.ds(0, SWEEPS), 1: pl.ds(LANES - SWEEPS, SWEEPS)}

    def corner(dr, dc):
        return (1 + dr) + (1 + dc) // 2

    def ends(dr, dc):
        if dr == 0:
            return columns.at[(1 + dc) // 2], sides.at[bands[dc]]
        if dc == 0:
            return ext.at[:, heights[dr]], ext.at[:, halos[dr]]
        return packed.at[corner(dr, dc)], corners.at[corner(dr, dc)]

    copies = {}
    for i, (dr, dc) in enumerate(DIRECTIONS):
        src, dst = ends(dr, dc)
        copies[dr, dc] = pltpu.make_async_remote_copy(
            src_ref=src,
            dst_ref=dst,
            send_sem=send_sem.at[i],
            recv_sem=recv_sem.at[i],
            device_id=(row + dr, col + dc),
            device_id_type=pl.DeviceIdType.MESH,
        )

    def encode(t):
        for load in loads[t]:
            load.wait()
        ext[t, :ROWS] = jnp.where(fg[t] == 1, jnp.exp2(key[t] * SCALE - SHIFT), BIG)

    low = lax.broadcasted_iota(jnp.int32, (PART, LANES), 1) < HALF
    for t, dc in ((0, -1), (3, 1)):
        encode(t)
        for dr, start in ((-1, 0), (1, ROWS - SWEEPS)):
            first = ext[t, start : start + PART]
            second = pltpu.roll(ext[t, start + PART : start + SWEEPS], HALF, 1)
            packed[corner(dr, dc)] = jnp.where(low, first, second) if dc < 0 else jnp.where(low, second, first)
        turned = ext[t, :ROWS].T
        columns[(1 + dc) // 2] = turned[:SWEEPS] if dc < 0 else turned[LANES - SWEEPS :]

    pl.semaphore_wait(barrier, count)
    early = row % 2 == 0
    for dr, dc in DIRECTIONS[:4]:
        pl.when(present(dr, dc) & (early if dr > 0 else jnp.logical_not(early)))(copies[dr, dc].start)
    for dr, dc in DIRECTIONS[4:6]:
        pl.when(present(dr, dc))(copies[dr, dc].start)
    for dr, dc in DIRECTIONS[:4]:
        pl.when(present(dr, dc) & (jnp.logical_not(early) if dr > 0 else early))(copies[dr, dc].start)
    for t in (1, 2):
        encode(t)
    for dr, dc in DIRECTIONS[6:]:
        pl.when(present(dr, dc))(copies[dr, dc].start)

    sides[SWEEPS : LANES - SWEEPS] = jnp.full((LANES - 2 * SWEEPS, ROWS), BIG, jnp.float32)
    for dr, dc in DIRECTIONS:

        @pl.when(jnp.logical_not(present(-dr, -dc)))
        def _():
            dst = ends(dr, dc)[1]
            dst[...] = jnp.full(dst.shape, BIG, jnp.float32)

    for dr, dc in DIRECTIONS[4:6]:
        pl.when(present(-dr, -dc))(copies[dr, dc].wait_recv)
    side[:ROWS] = sides[...].T
    for dr, dc in DIRECTIONS:
        pl.when(present(dr, dc))(copies[dr, dc].wait_send)
    for dr, dc in DIRECTIONS[6:] + DIRECTIONS[:4]:
        pl.when(present(-dr, -dc))(copies[dr, dc].wait_recv)
    for start, right, left in ((ROWS, 0, 1), (ROWS + SWEEPS, 2, 3)):
        side[start : start + PART] = jnp.where(low, corners[right], corners[left])
        other = jnp.where(low, corners[left], corners[right])
        side[start + PART : start + SWEEPS] = pltpu.roll(other, HALF, 1)


def sweep_kernel(ext, side, out, result, sem):
    bf16, f32 = jnp.bfloat16, jnp.float32
    big = jnp.full((BLOCKS, LANES), BIG, bf16)
    zero = jnp.zeros((BLOCKS, LANES), bf16)
    lane = lax.broadcasted_iota(jnp.int32, (BLOCKS, LANES), 1)
    phase = lane % LSTEPS

    def pick(value, lanes):
        return jnp.take_along_axis(value.astype(f32), lanes, axis=1).astype(bf16)

    def turn(first, last):
        return pltpu.roll(last, 1, 1), pltpu.roll(first, LANES - 1, 1)

    is_phase = [phase == p for p in range(LSTEPS)]
    tiles = []
    for k in range(STEPS):
        rows = pl.ds(k, BLOCKS, stride=STEPS)
        tiles.append([ext[t, rows, :].astype(bf16) for t in range(TILES)] + [side[rows, :].astype(bf16)])
    state = [[None] * LSTEPS for _ in range(STEPS)]
    for j in range(LSTEPS):
        for k in range(STEPS):
            value = tiles[k][0]
            for t in range(1, LSTEPS):
                value = jnp.where(is_phase[(j - 3 * t) % LSTEPS], tiles[k][t], value)
            state[k][j] = pick(value, (lane * LSTEPS + j) & (LANES - 1))
    mask = [[jnp.where(v >= EDGE, big, zero) for v in values] for values in state]

    def across(a, t):
        p, q = jnp.minimum(a[0], a[1]), jnp.minimum(a[2], a[3])
        return [
            jnp.minimum(t[0], p),
            jnp.minimum(p, a[2]),
            jnp.minimum(a[1], q),
            jnp.minimum(q, a[4]),
            jnp.minimum(jnp.minimum(a[3], a[4]), t[1]),
        ]

    turned = [turn(values[0], values[-1]) for values in state]
    for _ in range(SWEEPS):
        before = across(state[-1], turned[-1])
        here = top = across(state[0], turned[0])
        for k in range(0, STEPS, 2):
            after = across(state[k + 1], turned[k + 1])
            follow = across(state[k + 2], turned[k + 2]) if k + 2 < STEPS else top
            above = before if k else [pltpu.roll(b, 1, 0) for b in before]
            below = follow if k + 2 < STEPS else [pltpu.roll(f, BLOCKS - 1, 0) for f in follow]
            middle = [jnp.minimum(h, a) for h, a in zip(here, after)]
            state[k] = [jnp.maximum(jnp.minimum(a, m), c) for a, m, c in zip(above, middle, mask[k])]
            state[k + 1] = [jnp.maximum(jnp.minimum(m, b), c) for m, b, c in zip(middle, below, mask[k + 1])]
            turned[k] = turn(state[k][0], state[k][-1])
            turned[k + 1] = turn(state[k + 1][0], state[k + 1][-1])
            before, here = after, follow

    lanes = [(LANES * ((2 * (j - phase)) % LSTEPS) + lane) // LSTEPS for j in range(LSTEPS)]
    stores = []
    for k in range(STEPS):
        steps = [pick(state[k][j], lanes[j]) for j in range(LSTEPS)]
        more = (ROWS - 1 - k) // STEPS + 1 - 8
        for t in range(TILES):
            value = steps[0]
            for j in range(1, LSTEPS):
                value = jnp.where(is_phase[(j - 3 * t) % LSTEPS], steps[j], value)
            value = value.astype(f32)
            value = jnp.where(value >= EDGE, 0.0, jnp.log2(value) * (1 / SCALE) + SHIFT / SCALE)
            result[t, pl.ds(k, 8, stride=STEPS), :] = value[:8]
            result[t, pl.ds(k + 8 * STEPS, more, stride=STEPS), :] = value[8 : 8 + more]
    for t in range(TILES):
        stores.append(pltpu.make_async_copy(result.at[t], out.at[:, pl.ds(LANES * t, LANES)], sem.at[t]))
        stores[-1].start()
    for store in stores:
        store.wait()


def per_device(foreground, seed_keys):
    f32 = jnp.float32
    whole = pl.BlockSpec(memory_space=pltpu.VMEM)
    hbm = pl.BlockSpec(memory_space=pltpu.HBM)
    ext, side = pl.pallas_call(
        exchange_kernel,
        out_shape=[
            jax.ShapeDtypeStruct((TILES, WIDE, LANES), f32),
            jax.ShapeDtypeStruct((WIDE, LANES), f32),
        ],
        in_specs=[hbm] * 2,
        out_specs=[whole] * 2,
        scratch_shapes=[
            pltpu.VMEM((LANES, ROWS), f32),
            pltpu.VMEM((4, PART, LANES), f32),
            pltpu.VMEM((TILES, ROWS, LANES), jnp.int32),
            pltpu.VMEM((TILES, ROWS, LANES), f32),
            pltpu.VMEM((2, SWEEPS, ROWS), f32),
            pltpu.VMEM((4, PART, LANES), f32),
            pltpu.SemaphoreType.DMA((2, TILES)),
            pltpu.SemaphoreType.DMA((8,)),
            pltpu.SemaphoreType.DMA((8,)),
        ],
        compiler_params=pltpu.CompilerParams(
            collective_id=0, has_side_effects=True, vmem_limit_bytes=16 * 2**20
        ),
        name="exchange",
    )(
        pltpu.with_memory_space_constraint(foreground, pltpu.HBM),
        pltpu.with_memory_space_constraint(seed_keys, pltpu.HBM),
    )
    return pl.pallas_call(
        sweep_kernel,
        out_shape=jax.ShapeDtypeStruct((ROWS, TILES * LANES), f32),
        in_specs=[whole] * 2,
        out_specs=hbm,
        scratch_shapes=[
            pltpu.VMEM((TILES, ROWS, LANES), f32),
            pltpu.SemaphoreType.DMA((TILES,)),
        ],
        compiler_params=pltpu.CompilerParams(vmem_limit_bytes=16 * 2**20),
        name="sweeps",
    )(ext, side)


def solution(mesh):
    placed = (P("row", "col"), P("row", "col"))
    return jax.shard_map(
        per_device, mesh=mesh, in_specs=placed, out_specs=P("row", "col"), check_vma=False
    )
```
